256 devices in a mesh: py: 16 (over z_lo, y_hi, x), px: 4 (over z_hi), pz: 4 (over y_lo, core).
Axes of the slice: x: 4, y: 4 (y_hi: 2, y_lo: 2; y = y_hi * 2 + y_lo), z: 8 (z_hi: 4, z_lo: 2; z = z_hi * 2 + z_lo), core: 2. Of those that a mesh axis runs over, the one named last changes fastest.
Arguments:
- field_now: float32 [128, 64, 256, 128], P('py', 'px', 'pz'), may hold values from 0.2 to 1.8
- earlier: float32 [128, 64, 256, 128], P('py', 'px', 'pz'), may hold values from 0.2 to 1.8
- speed_square: float32 [128, 64, 256, 128], P('py', 'px', 'pz'), may hold values from 0.05 to 0.3
Outputs:
- column_sum: float32 [128, 64, 256, 128], P('py', 'px', 'pz')
- field_now_end: float32 [128, 64, 256, 128], P('py', 'px', 'pz')
The draws below stay inside these ranges and needn't reach their ends.
All inputs are finite; a program needn't handle non-finite values.
Results may differ from the reference program's by a relative error of at most 0.00002.
Values sent between devices are 32-bit elements; how exact they have to be, the bound alone decides.
A program may use at most 128 MiB of HBM per device.

```python
import jax
import jax.numpy as jnp
from jax import lax

GRID_J = 128
GRID_I = 64
GRID_K = 256
LEVELS = 128
STEPS = 4


def shard_levels(key, extent, split, low, top_value):
    level = 1.0
    for position, shards_of in split:
        heights = jax.random.uniform(jax.random.fold_in(jax.random.fold_in(key, 6), position), (shards_of,), jnp.float32, low / len(split), top_value / len(split))
        level = level * jnp.repeat(jnp.exp(heights), extent[position] // shards_of).reshape((-1,) + (1,) * (len(extent) - 1 - position))
    return level


def setup_inputs(seed: int = 0) -> dict:
    seeds = jax.random.split(jax.random.key(seed), 4)
    field_now = jnp.clip(0.2 + 1.5999999 * jax.random.uniform(seeds[0], (GRID_J, GRID_I, GRID_K, LEVELS), jnp.float32) ** shard_levels(seeds[0], (GRID_J, GRID_I, GRID_K, LEVELS), ((0, 16), (1, 4), (2, 4)), -0.2, 0.2), 0.2, 1.8)
    earlier = jnp.clip(0.2 + 1.5999999 * jax.random.uniform(seeds[1], (GRID_J, GRID_I, GRID_K, LEVELS), jnp.float32) ** shard_levels(seeds[1], (GRID_J, GRID_I, GRID_K, LEVELS), ((0, 16), (1, 4), (2, 4)), -0.2, 0.2), 0.2, 1.8)
    speed_square = jnp.clip(0.05 + 0.25 * jax.random.uniform(seeds[2], (GRID_J, GRID_I, GRID_K, LEVELS), jnp.float32) ** shard_levels(seeds[2], (GRID_J, GRID_I, GRID_K, LEVELS), ((0, 16), (1, 4), (2, 4)), -0.2, 0.2), 0.05, 0.3)
    return dict(field_now=field_now, earlier=earlier, speed_square=speed_square)


def without_rim(values, dims):
    for dim in dims:
        values = lax.slice_in_dim(values, 1, values.shape[dim] - 1, axis=dim)
    return values


def shifted_cells(values, dim, start, dims):
    others = [other for other in dims if other != dim]
    values = without_rim(values, others)
    return lax.slice_in_dim(values, start, start + values.shape[dim] - 2, axis=dim)


def march_step(padded, before, speed_square):
    middle = without_rim(padded, (0, 1, 2))
    lower = [shifted_cells(padded, dim, 0, (0, 1, 2)) for dim in (0, 1, 2)]
    upper = [shifted_cells(padded, dim, 2, (0, 1, 2)) for dim in (0, 1, 2)]
    spread = lower[0] + upper[0] + lower[1] + upper[1] + lower[2] + upper[2] - 6.0 * middle
    return 2.0 * middle - before + speed_square * spread


def reference(field_now, earlier, speed_square):
    for step in range(STEPS):
        later = march_step(jnp.pad(field_now, ((1, 1), (1, 1), (1, 1), (0, 0)), mode="wrap"), earlier, speed_square)
        earlier, field_now = field_now, later
    column_sum = jnp.cumsum(field_now, axis=0) / GRID_J
    return column_sum, field_now
```

```python
import functools

import jax
import jax.numpy as jnp
from jax import lax
from jax.experimental import pallas as pl
from jax.experimental.pallas import tpu as pltpu
from jax.sharding import PartitionSpec as P

STEPS = 4
MESH = pl.DeviceIdType.MESH
PAD = 8
CHUNKS = 4
ORDER = (0, 3, 1, 2)
JUP, JDOWN, IUP, IDOWN = range(4)


def march_kernel(
    sizes, u_hbm, e_hbm, c_hbm, end_hbm, below_hbm,
    field, speed, k_out, k_in, total, gathered, prefix,
    load_sem, send_sem, recv_sem, k_send_sem, k_recv_sem,
    out_sem, own_sem, t_send_sem, t_recv_sem, p_send_sem, p_recv_sem,
):
    ny, nx, nz = sizes
    nj, ni, nk, _ = u_hbm.shape
    kc = nk // CHUNKS
    y, x, z = lax.axis_index("py"), lax.axis_index("px"), lax.axis_index("pz")
    up = {"py": lax.rem(y + 1, ny), "px": lax.rem(x + 1, nx), "pz": lax.rem(z + 1, nz)}
    down = {"py": lax.rem(y + ny - 1, ny), "px": lax.rem(x + nx - 1, nx), "pz": lax.rem(z + nz - 1, nz)}

    def inner(piece):
        return pl.ds(piece * kc, kc)

    def padded(piece, shift=0):
        return pl.ds(PAD + piece * kc + shift, kc)

    def load(which, piece):
        block = (pl.ds(1, nj), pl.ds(1, ni), padded(piece))
        cells = (slice(None), slice(None), inner(piece))
        source = (u_hbm, e_hbm, c_hbm)[which].at[cells]
        target = speed.at[cells] if which == 2 else field.at[(which, *block)]
        return pltpu.make_async_copy(source, target, load_sem.at[which, piece])

    def face(step, piece, side):
        slot = step % 2
        rows = padded(piece)
        i_all, j_all = pl.ds(1, ni), pl.ds(1, nj)
        here = {
            JUP: (slot, nj, i_all, rows),
            JDOWN: (slot, 1, i_all, rows),
            IUP: (slot, j_all, ni, rows),
            IDOWN: (slot, j_all, 1, rows),
        }[side]
        there = {
            JUP: (slot, 0, i_all, rows),
            JDOWN: (slot, nj + 1, i_all, rows),
            IUP: (slot, j_all, 0, rows),
            IDOWN: (slot, j_all, ni + 1, rows),
        }[side]
        axis = "py" if side in (JUP, JDOWN) else "px"
        to = (up if side in (JUP, IUP) else down)[axis]
        if step == 0:
            rows = inner(piece)
            source = u_hbm.at[
                {
                    JUP: (nj - 1, slice(None), rows),
                    JDOWN: (0, slice(None), rows),
                    IUP: (slice(None), ni - 1, rows),
                    IDOWN: (slice(None), 0, rows),
                }[side]
            ]
        else:
            source = field.at[here]
        return pltpu.make_async_remote_copy(
            src_ref=source, dst_ref=field.at[there],
            send_sem=send_sem.at[step, piece, side], recv_sem=recv_sem.at[step, piece, side],
            device_id={axis: to}, device_id_type=MESH,
        )

    def k_face(step, high):
        return pltpu.make_async_remote_copy(
            src_ref=k_out.at[step % 2, high], dst_ref=k_in.at[step % 2, high],
            send_sem=k_send_sem.at[step, high], recv_sem=k_recv_sem.at[step, high],
            device_id={"pz": (up if high else down)["pz"]}, device_id_type=MESH,
        )

    def send_k_face(step, high):
        slot = step % 2
        row = PAD + (nk - 1 if high else 0)

        def gather(j, _):
            for i in range(ni):
                k_out[slot, high, j, pl.ds(i, 1)] = field[slot, j + 1, i + 1, pl.ds(row, 1)]
            return 0

        lax.fori_loop(0, nj, gather, 0)
        k_face(step, high).start()

    def take_k_face(step, high):
        slot = step % 2
        row = PAD - 1 if high else PAD + nk
        k_face(step, high).wait_recv()

        def scatter(j, _):
            for i in range(ni):
                field[slot, j + 1, i + 1, pl.ds(row, 1)] = k_in[slot, high, j, pl.ds(i, 1)]
            return 0

        lax.fori_loop(0, nj, scatter, 0)

    def advance(step, piece):
        now, later = step % 2, (step + 1) % 2
        rows = padded(piece)
        lower, upper = padded(piece, -1), padded(piece, 1)

        def column(i, _):
            cells = [field[now, j, i + 1, rows] for j in range(nj + 2)]
            amount = None
            for j in range(1, nj + 1):
                middle = cells[j]
                spread = cells[j - 1] + cells[j + 1]
                spread = spread + (field[now, j, i, rows] + field[now, j, i + 2, rows])
                spread = spread + (field[now, j, i + 1, lower] + field[now, j, i + 1, upper])
                spread = spread - 6.0 * middle
                value = 2.0 * middle - field[later, j, i + 1, rows] + speed[j - 1, i, inner(piece)] * spread
                field[later, j, i + 1, rows] = value
                amount = value if amount is None else amount + value
            if step == STEPS - 1:
                total[i, inner(piece)] = amount
            return 0

        lax.fori_loop(0, ni, column, 0)

    def end_copy(piece):
        return pltpu.make_async_copy(
            field.at[STEPS % 2, pl.ds(1, nj), pl.ds(1, ni), padded(piece)], end_hbm.at[:, :, inner(piece)], out_sem.at[piece]
        )

    def total_copy(piece, away):
        to = lax.rem(y + away, ny)
        return pltpu.make_async_remote_copy(
            src_ref=total.at[to, inner(piece)], dst_ref=gathered.at[piece, y],
            send_sem=t_send_sem.at[piece], recv_sem=t_recv_sem.at[piece],
            device_id={"py": to}, device_id_type=MESH,
        )

    def prefix_copy(piece, away):
        to = lax.rem(y + away, ny)
        return pltpu.make_async_remote_copy(
            src_ref=prefix.at[piece, to], dst_ref=below_hbm.at[y, inner(piece)],
            send_sem=p_send_sem.at[piece], recv_sem=p_recv_sem.at[piece],
            device_id={"py": to}, device_id_type=MESH,
        )

    def own_prefix(piece):
        return pltpu.make_async_copy(prefix.at[piece, y], below_hbm.at[y, inner(piece)], own_sem.at[piece])

    def others(sem):
        return pltpu.make_async_copy(gathered.at[0, pl.ds(0, ny - 1)], gathered.at[0, pl.ds(0, ny - 1)], sem)

    def to_all(copy, piece):
        def one(away, _):
            copy(piece, away).start()
            return 0

        lax.fori_loop(1, ny, one, 0)

    def send_totals(piece):
        to_all(total_copy, piece)

    def send_prefixes(piece):
        others(t_recv_sem.at[piece]).wait()
        gathered[piece, y] = total[y, inner(piece)]

        def add(n, so_far):
            prefix[piece, n] = so_far
            return so_far + gathered[piece, n]

        lax.fori_loop(0, ny, add, jnp.zeros(gathered.shape[2:], jnp.float32))
        to_all(prefix_copy, piece)
        own_prefix(piece).start()

    for piece in ORDER:
        load(0, piece).start()
    barrier = pltpu.get_barrier_semaphore()

    def greet(away, _):
        pl.semaphore_signal(barrier, inc=1, device_id={"py": lax.rem(y + away, ny)}, device_id_type=MESH)
        return 0

    for axis in ("px", "pz"):
        for near in (up, down):
            pl.semaphore_signal(barrier, inc=1, device_id={axis: near[axis]}, device_id_type=MESH)
    lax.fori_loop(1, ny, greet, 0)
    pl.semaphore_wait(barrier, ny - 1 + 4)

    for piece in ORDER:
        for side in range(4):
            face(0, piece, side).start()
    for piece in ORDER:
        for which in (1, 2):
            load(which, piece).start()
    for piece in ORDER:
        load(0, piece).wait()
        if piece == 0:
            send_k_face(0, 0)
        if piece == CHUNKS - 1:
            send_k_face(0, 1)

    for step in range(STEPS):
        for at, piece in enumerate(ORDER):
            if step == 0:
                for which in (1, 2):
                    load(which, piece).wait()
            if piece == 0:
                take_k_face(step, 1)
            if piece == CHUNKS - 1:
                take_k_face(step, 0)
            for side in range(4):
                if step >= 1:
                    face(step - 1, piece, side).wait_send()
                face(step, piece, side).wait_recv()
            advance(step, piece)
            if step < STEPS - 1:
                for side in range(4):
                    face(step + 1, piece, side).start()
                for high, owner in ((0, 0), (1, CHUNKS - 1)):
                    if piece == owner:
                        if step >= 1:
                            k_face(step - 1, high).wait_send()
                        send_k_face(step + 1, high)
            else:
                end_copy(piece).start()
                send_totals(piece)
                if at >= 2:
                    send_prefixes(ORDER[at - 2])
    for piece in ORDER[2:]:
        send_prefixes(piece)
    for piece in ORDER:
        for side in range(4):
            face(STEPS - 1, piece, side).wait_send()
        end_copy(piece).wait()
        own_prefix(piece).wait()
        others(t_send_sem.at[piece]).wait()
        others(p_send_sem.at[piece]).wait()
        others(p_recv_sem.at[piece]).wait()
    for step in (STEPS - 2, STEPS - 1):
        for high in (0, 1):
            k_face(step, high).wait_send()


def sums_kernel(scale, field_ref, below_ref, sums_ref, end_ref):
    so_far = below_ref[...]
    for j in range(field_ref.shape[0]):
        value = field_ref[j]
        end_ref[j] = value
        so_far = so_far + value
        sums_ref[j] = so_far * scale


def local(sizes, field_now, earlier, speed_square):
    nj, ni, nk, lanes = field_now.shape
    kc = nk // CHUNKS
    f32 = jnp.float32
    dma = pltpu.SemaphoreType.DMA
    end, below = pl.pallas_call(
        functools.partial(march_kernel, sizes),
        out_shape=(jax.ShapeDtypeStruct(field_now.shape, f32), jax.ShapeDtypeStruct((ni, nk, lanes), f32)),
        in_specs=[pl.BlockSpec(memory_space=pl.ANY)] * 3,
        out_specs=[pl.BlockSpec(memory_space=pl.ANY)] * 2,
        scratch_shapes=[
            pltpu.VMEM((2, nj + 2, ni + 2, nk + 2 * PAD, lanes), f32),
            pltpu.VMEM((nj, ni, nk, lanes), f32),
            pltpu.VMEM((2, 2, nj, ni, lanes), f32),
            pltpu.VMEM((2, 2, nj, ni, lanes), f32),
            pltpu.VMEM((ni, nk, lanes), f32),
            pltpu.VMEM((CHUNKS, ni, kc, lanes), f32),
            pltpu.VMEM((CHUNKS, ni, kc, lanes), f32),
            dma((3, CHUNKS)),
            dma((STEPS, CHUNKS, 4)),
            dma((STEPS, CHUNKS, 4)),
            dma((STEPS, 2)),
            dma((STEPS, 2)),
            dma((CHUNKS,)),
            dma((CHUNKS,)),
            dma((CHUNKS,)),
            dma((CHUNKS,)),
            dma((CHUNKS,)),
            dma((CHUNKS,)),
        ],
        compiler_params=pltpu.CompilerParams(
            collective_id=0, has_side_effects=True, vmem_limit_bytes=48 * 1024 * 1024
        ),
        name="march",
    )(field_now, earlier, speed_square)
    rows = 2
    block = pl.BlockSpec((nj, rows, nk, lanes), lambda n: (0, n, 0, 0))
    sums, end = pl.pallas_call(
        functools.partial(sums_kernel, 1.0 / (nj * sizes[0])),
        grid=(ni // rows,),
        out_shape=(jax.ShapeDtypeStruct(field_now.shape, f32),) * 2,
        in_specs=[block, pl.BlockSpec((rows, nk, lanes), lambda n: (n, 0, 0))],
        out_specs=[block, block],
        name="sums",
    )(end, below)
    return sums, end


def solution(mesh):
    spec = P("py", "px", "pz", None)
    sizes = tuple(mesh.shape[axis] for axis in ("py", "px", "pz"))
    return jax.shard_map(
        functools.partial(local, sizes),
        mesh=mesh,
        in_specs=(spec, spec, spec),
        out_specs=(spec, spec),
        check_vma=False,
    )
```

```python
import functools

import jax
import jax.numpy as jnp
from jax import lax
from jax.experimental import pallas as pl
from jax.experimental.pallas import tpu as pltpu
from jax.sharding import PartitionSpec as P

STEPS = 4
MESH = pl.DeviceIdType.MESH
PAD = 8
CHUNKS = 4
ORDER = (0, 3, 1, 2)
JUP, JDOWN, IUP, IDOWN = SIDES = range(4)
STRAIGHT, ROUND, BESIDE = PARTS = ((0, 5), (5, 6), (11, 5))


def march_kernel(
    sizes, u_hbm, e_hbm, c_hbm, end_hbm, below_hbm,
    field, speed, k_out, k_in, total, gathered, prefix, passing,
    load_sem, send_sem, recv_sem, k_send_sem, k_recv_sem, pass_send_sem, pass_recv_sem,
    out_sem, own_sem, t_send_sem, t_recv_sem, p_send_sem, p_recv_sem,
):
    ny, nx, nz = sizes
    nj, ni, nk, _ = u_hbm.shape
    kc = nk // CHUNKS
    y, x, z = lax.axis_index("py"), lax.axis_index("px"), lax.axis_index("pz")
    up = {"py": lax.rem(y + 1, ny), "px": lax.rem(x + 1, nx), "pz": lax.rem(z + 1, nz)}
    down = {"py": lax.rem(y + ny - 1, ny), "px": lax.rem(x + nx - 1, nx), "pz": lax.rem(z + nz - 1, nz)}

    def inner(piece):
        return pl.ds(piece * kc, kc)

    def padded(piece, shift=0):
        return pl.ds(PAD + piece * kc + shift, kc)

    def load(which, piece):
        block = (pl.ds(1, nj), pl.ds(1, ni), padded(piece))
        cells = (slice(None), slice(None), inner(piece))
        source = (u_hbm, e_hbm, c_hbm)[which].at[cells]
        target = speed.at[cells] if which == 2 else field.at[(which, *block)]
        return pltpu.make_async_copy(source, target, load_sem.at[which, piece])

    run, half = ny // 2, ny // 4
    place = lax.rem(y, run)
    ends = {JUP: place == run - 1, JDOWN: place == 0}
    away = {(JUP, ROUND): 1 - half, (JUP, BESIDE): -1, (JDOWN, ROUND): half - 1, (JDOWN, BESIDE): 1}

    def face(step, piece, side, part=None, passed=False):
        slot = step % 2
        rows = padded(piece)
        first, count = part or (0, ni)
        i_all, j_all = pl.ds(1 + first, count), pl.ds(1, nj)
        along_j, high = side in (JUP, JDOWN), side in (JUP, IUP)
        if along_j:
            here = (slot, nj if high else 1, i_all, rows)
            there = (slot, 0 if high else nj + 1, i_all, rows)
        else:
            here = (slot, j_all, ni if high else 1, rows)
            there = (slot, j_all, 0 if high else ni + 1, rows)
        axis = "py" if along_j else "px"
        to = (up if high else down)[axis]
        source, target = field.at[here], field.at[there]
        arrived = recv_sem.at[step, piece, side]
        if step == 0:
            rows = inner(piece)
            if along_j:
                source = u_hbm.at[nj - 1 if high else 0, pl.ds(first, count), rows]
            else:
                source = u_hbm.at[:, ni - 1 if high else 0, rows]
        if passed:
            to = y + away[side, part]
            target, arrived = passing.at[step, piece, pl.ds(0, count)], pass_recv_sem.at[step, piece]
        return pltpu.make_async_remote_copy(
            src_ref=source, dst_ref=target, send_sem=send_sem.at[step, piece, side], recv_sem=arrived,
            device_id={axis: to}, device_id_type=MESH,
        )

    def pass_on(step, piece, side, part):
        first, count = part
        high = side == JUP
        to = lax.rem(y - away[side, part] + (1 if high else ny - 1), ny)
        there = (step % 2, 0 if high else nj + 1, pl.ds(1 + first, count), padded(piece))
        return pltpu.make_async_remote_copy(
            src_ref=passing.at[step, piece, pl.ds(0, count)], dst_ref=field.at[there],
            send_sem=pass_send_sem.at[step, piece], recv_sem=recv_sem.at[step, piece, side],
            device_id={"py": to}, device_id_type=MESH,
        )

    def send_faces(step, piece):
        for side in SIDES:
            if side not in ends:
                face(step, piece, side).start()
                continue

            @pl.when(ends[side])
            def _():
                for part in (ROUND, BESIDE):
                    face(step, piece, side, part, passed=True).start()
                face(step, piece, side, STRAIGHT).start()

            @pl.when(jnp.logical_not(ends[side]))
            def _():
                face(step, piece, side).start()

    def as_relay(act):
        for (side, part), steps in away.items():
            at = (run - 1 if side == JUP else 0) + steps
            pl.when(place == at)(functools.partial(act, side, part))

    def relay(step, piece):
        def act(side, part):
            face(step, piece, side, part, passed=True).wait_recv()
            pass_on(step, piece, side, part).start()

        as_relay(act)

    def k_face(step, high):
        return pltpu.make_async_remote_copy(
            src_ref=k_out.at[step % 2, high], dst_ref=k_in.at[step % 2, high],
            send_sem=k_send_sem.at[step, high], recv_sem=k_recv_sem.at[step, high],
            device_id={"pz": (up if high else down)["pz"]}, device_id_type=MESH,
        )

    def send_k_face(step, high):
        slot = step % 2
        row = PAD + (nk - 1 if high else 0)

        def gather(j, _):
            for i in range(ni):
                k_out[slot, high, j, pl.ds(i, 1)] = field[slot, j + 1, i + 1, pl.ds(row, 1)]
            return 0

        lax.fori_loop(0, nj, gather, 0)
        k_face(step, high).start()

    def take_k_face(step, high):
        slot = step % 2
        row = PAD - 1 if high else PAD + nk
        k_face(step, high).wait_recv()

        def scatter(j, _):
            for i in range(ni):
                field[slot, j + 1, i + 1, pl.ds(row, 1)] = k_in[slot, high, j, pl.ds(i, 1)]
            return 0

        lax.fori_loop(0, nj, scatter, 0)

    def advance(step, piece):
        now, later = step % 2, (step + 1) % 2
        rows = padded(piece)
        lower, upper = padded(piece, -1), padded(piece, 1)

        def column(i, _):
            cells = [field[now, j, i + 1, rows] for j in range(nj + 2)]
            amount = None
            for j in range(1, nj + 1):
                middle = cells[j]
                spread = cells[j - 1] + cells[j + 1]
                spread = spread + (field[now, j, i, rows] + field[now, j, i + 2, rows])
                spread = spread + (field[now, j, i + 1, lower] + field[now, j, i + 1, upper])
                spread = spread - 6.0 * middle
                value = 2.0 * middle - field[later, j, i + 1, rows] + speed[j - 1, i, inner(piece)] * spread
                field[later, j, i + 1, rows] = value
                amount = value if amount is None else amount + value
            if step == STEPS - 1:
                total[i, inner(piece)] = amount
            return 0

        lax.fori_loop(0, ni, column, 0)

    def end_copy(piece):
        return pltpu.make_async_copy(
            field.at[STEPS % 2, pl.ds(1, nj), pl.ds(1, ni), padded(piece)], end_hbm.at[:, :, inner(piece)], out_sem.at[piece]
        )

    def total_copy(piece, away):
        to = lax.rem(y + away, ny)
        return pltpu.make_async_remote_copy(
            src_ref=total.at[to, inner(piece)], dst_ref=gathered.at[piece, y],
            send_sem=t_send_sem.at[piece], recv_sem=t_recv_sem.at[piece],
            device_id={"py": to}, device_id_type=MESH,
        )

    def prefix_copy(piece, away):
        to = lax.rem(y + away, ny)
        return pltpu.make_async_remote_copy(
            src_ref=prefix.at[piece, to], dst_ref=below_hbm.at[y, inner(piece)],
            send_sem=p_send_sem.at[piece], recv_sem=p_recv_sem.at[piece],
            device_id={"py": to}, device_id_type=MESH,
        )

    def own_prefix(piece):
        return pltpu.make_async_copy(prefix.at[piece, y], below_hbm.at[y, inner(piece)], own_sem.at[piece])

    def others(sem):
        return pltpu.make_async_copy(gathered.at[0, pl.ds(0, ny - 1)], gathered.at[0, pl.ds(0, ny - 1)], sem)

    def to_all(copy, piece):
        def one(away, _):
            copy(piece, away).start()
            return 0

        lax.fori_loop(1, ny, one, 0)

    def send_totals(piece):
        to_all(total_copy, piece)

    def send_prefixes(piece):
        others(t_recv_sem.at[piece]).wait()
        gathered[piece, y] = total[y, inner(piece)]

        def add(n, so_far):
            prefix[piece, n] = so_far
            return so_far + gathered[piece, n]

        lax.fori_loop(0, ny, add, jnp.zeros(gathered.shape[2:], jnp.float32))
        to_all(prefix_copy, piece)
        own_prefix(piece).start()

    for piece in ORDER:
        load(0, piece).start()
    barrier = pltpu.get_barrier_semaphore()

    def greet(away, _):
        pl.semaphore_signal(barrier, inc=1, device_id={"py": lax.rem(y + away, ny)}, device_id_type=MESH)
        return 0

    for axis in ("px", "pz"):
        for near in (up, down):
            pl.semaphore_signal(barrier, inc=1, device_id={axis: near[axis]}, device_id_type=MESH)
    lax.fori_loop(1, ny, greet, 0)
    pl.semaphore_wait(barrier, ny - 1 + 4)

    for piece in ORDER:
        send_faces(0, piece)
    for piece in ORDER:
        for which in (1, 2):
            load(which, piece).start()
    for piece in ORDER:
        load(0, piece).wait()
        if piece == 0:
            send_k_face(0, 0)
        if piece == CHUNKS - 1:
            send_k_face(0, 1)

    for step in range(STEPS):
        for at, piece in enumerate(ORDER):
            if step == 0:
                for which in (1, 2):
                    load(which, piece).wait()
            if piece == 0:
                take_k_face(step, 1)
            if piece == CHUNKS - 1:
                take_k_face(step, 0)
            relay(step, piece)
            for side in SIDES:
                if step >= 1:
                    face(step - 1, piece, side).wait_send()
                face(step, piece, side).wait_recv()
            advance(step, piece)
            if step < STEPS - 1:
                send_faces(step + 1, piece)
                for high, owner in ((0, 0), (1, CHUNKS - 1)):
                    if piece == owner:
                        if step >= 1:
                            k_face(step - 1, high).wait_send()
                        send_k_face(step + 1, high)
            else:
                end_copy(piece).start()
                send_totals(piece)
                if at >= 2:
                    send_prefixes(ORDER[at - 2])
    for piece in ORDER[2:]:
        send_prefixes(piece)
    for piece in ORDER:
        for side in SIDES:
            face(STEPS - 1, piece, side).wait_send()
        end_copy(piece).wait()
        own_prefix(piece).wait()
        others(t_send_sem.at[piece]).wait()
        others(p_send_sem.at[piece]).wait()
        others(p_recv_sem.at[piece]).wait()
    for step in (STEPS - 2, STEPS - 1):
        for high in (0, 1):
            k_face(step, high).wait_send()

    def passed_on(side, part):
        for step in range(STEPS):
            for piece in ORDER:
                pass_on(step, piece, side, part).wait_send()

    as_relay(passed_on)


def sums_kernel(scale, field_ref, below_ref, sums_hbm, end_hbm, sums, sem):
    nj, ni = field_ref.shape[:2]
    ends = pltpu.make_async_copy(field_ref, end_hbm, sem.at[ni])
    ends.start()

    def put(i):
        return pltpu.make_async_copy(sums.at[:, i], sums_hbm.at[:, i], sem.at[i])

    def row(i, _):
        so_far = below_ref[i]
        for j in range(nj):
            so_far = so_far + field_ref[j, i]
            sums[j, i] = so_far * scale
        put(i).start()
        return 0

    lax.fori_loop(0, ni, row, 0)

    def written(i, _):
        put(i).wait()
        return 0

    lax.fori_loop(0, ni, written, 0)
    ends.wait()


def local(sizes, field_now, earlier, speed_square):
    nj, ni, nk, lanes = field_now.shape
    kc = nk // CHUNKS
    f32 = jnp.float32
    dma = pltpu.SemaphoreType.DMA
    end, below = pl.pallas_call(
        functools.partial(march_kernel, sizes),
        out_shape=(jax.ShapeDtypeStruct(field_now.shape, f32), jax.ShapeDtypeStruct((ni, nk, lanes), f32)),
        in_specs=[pl.BlockSpec(memory_space=pl.ANY)] * 3,
        out_specs=[pl.BlockSpec(memory_space=pl.ANY)] * 2,
        scratch_shapes=[
            pltpu.VMEM((2, nj + 2, ni + 2, nk + 2 * PAD, lanes), f32),
            pltpu.VMEM((nj, ni, nk, lanes), f32),
            pltpu.VMEM((2, 2, nj, ni, lanes), f32),
            pltpu.VMEM((2, 2, nj, ni, lanes), f32),
            pltpu.VMEM((ni, nk, lanes), f32),
            pltpu.VMEM((CHUNKS, ni, kc, lanes), f32),
            pltpu.VMEM((CHUNKS, ni, kc, lanes), f32),
            pltpu.VMEM((STEPS, CHUNKS, max(ROUND[1], BESIDE[1]), kc, lanes), f32),
            dma((3, CHUNKS)),
            dma((STEPS, CHUNKS, len(SIDES))),
            dma((STEPS, CHUNKS, len(SIDES))),
            dma((STEPS, 2)),
            dma((STEPS, 2)),
            dma((STEPS, CHUNKS)),
            dma((STEPS, CHUNKS)),
            dma((CHUNKS,)),
            dma((CHUNKS,)),
            dma((CHUNKS,)),
            dma((CHUNKS,)),
            dma((CHUNKS,)),
            dma((CHUNKS,)),
        ],
        compiler_params=pltpu.CompilerParams(
            collective_id=0, has_side_effects=True, vmem_limit_bytes=48 * 1024 * 1024
        ),
        name="march",
    )(field_now, earlier, speed_square)
    sums, end = pl.pallas_call(
        functools.partial(sums_kernel, 1.0 / (nj * sizes[0])),
        out_shape=(jax.ShapeDtypeStruct(field_now.shape, f32),) * 2,
        in_specs=[pl.BlockSpec(memory_space=pltpu.VMEM)] * 2,
        out_specs=[pl.BlockSpec(memory_space=pl.ANY)] * 2,
        scratch_shapes=[pltpu.VMEM(field_now.shape, f32), dma((ni + 1,))],
        compiler_params=pltpu.CompilerParams(vmem_limit_bytes=16 * 1024 * 1024),
        name="sums",
    )(end, below)
    return sums, end


def solution(mesh):
    spec = P("py", "px", "pz", None)
    sizes = tuple(mesh.shape[axis] for axis in ("py", "px", "pz"))
    return jax.shard_map(
        functools.partial(local, sizes),
        mesh=mesh,
        in_specs=(spec, spec, spec),
        out_specs=(spec, spec),
        check_vma=False,
    )
```

```python
import functools

import jax
import jax.numpy as jnp
from jax import lax
from jax.experimental import pallas as pl
from jax.experimental.pallas import tpu as pltpu
from jax.sharding import PartitionSpec as P

STEPS = 4
MESH = pl.DeviceIdType.MESH
PAD = 8
CHUNKS = 4
ORDER = (1, 2, 0, 3)
JUP, JDOWN, IUP, IDOWN = SIDES = range(4)
STRAIGHT, ROUND, BESIDE = PARTS = ((0, 5), (5, 6), (11, 5))


def march_kernel(
    sizes, u_hbm, e_hbm, c_hbm, end_hbm, below_hbm,
    field, speed, k_out, k_in, total, gathered, prefix, passing,
    load_sem, send_sem, recv_sem, i_recv_sem, k_send_sem, k_recv_sem, pass_send_sem, pass_recv_sem,
    out_sem, t_send_sem, t_recv_sem, p_send_sem, p_recv_sem,
):
    ny, nx, nz = sizes
    nj, ni, nk, _ = u_hbm.shape
    kc = nk // CHUNKS
    y, x, z = lax.axis_index("py"), lax.axis_index("px"), lax.axis_index("pz")
    up = {"py": lax.rem(y + 1, ny), "px": lax.rem(x + 1, nx), "pz": lax.rem(z + 1, nz)}
    down = {"py": lax.rem(y + ny - 1, ny), "px": lax.rem(x + nx - 1, nx), "pz": lax.rem(z + nz - 1, nz)}

    def inner(piece):
        return pl.ds(piece * kc, kc)

    def padded(piece, shift=0):
        return pl.ds(PAD + piece * kc + shift, kc)

    def load(which, piece):
        block = (pl.ds(1, nj), pl.ds(1, ni), padded(piece))
        cells = (slice(None), slice(None), inner(piece))
        source = (u_hbm, e_hbm, c_hbm)[which].at[cells]
        target = speed.at[cells] if which == 2 else field.at[(which, *block)]
        return pltpu.make_async_copy(source, target, load_sem.at[which])

    run, half = ny // 2, ny // 4
    place = lax.rem(y, run)
    ends = {JUP: place == run - 1, JDOWN: place == 0}
    away = {(JUP, ROUND): 1 - half, (JUP, BESIDE): -half - 1, (JDOWN, ROUND): half - 1, (JDOWN, BESIDE): half + 1}

    def loaded(which):
        pltpu.make_async_copy(c_hbm, speed, load_sem.at[which]).wait()

    def face(step, piece, side, part=None, passed=False):
        slot = step % 2
        rows = padded(piece)
        first, count = part or (0, ni)
        i_all, j_all = pl.ds(1 + first, count), pl.ds(1, nj)
        along_j, high = side in (JUP, JDOWN), side in (JUP, IUP)
        if along_j:
            here = (slot, nj if high else 1, i_all, rows)
            there = (slot, 0 if high else nj + 1, i_all, rows)
        else:
            here = (slot, j_all, ni if high else 1, rows)
            there = (slot, j_all, 0 if high else ni + 1, rows)
        axis = "py" if along_j else "px"
        to = (up if high else down)[axis]
        source, target = field.at[here], field.at[there]
        arrived = (recv_sem if along_j else i_recv_sem).at[step % 2, piece]
        if passed:
            to = y + away[side, part]
            target, arrived = passing.at[step, piece, pl.ds(0, count)], pass_recv_sem.at[step % 2, piece]
        return pltpu.make_async_remote_copy(
            src_ref=source, dst_ref=target, send_sem=send_sem.at[step % 2, piece], recv_sem=arrived,
            device_id={axis: to}, device_id_type=MESH,
        )

    def pass_on(step, piece, side, part):
        first, count = part
        high = side == JUP
        to = lax.rem(y - away[side, part] + (1 if high else ny - 1), ny)
        there = (step % 2, 0 if high else nj + 1, pl.ds(1 + first, count), padded(piece))
        return pltpu.make_async_remote_copy(
            src_ref=passing.at[step, piece, pl.ds(0, count)], dst_ref=field.at[there],
            send_sem=pass_send_sem.at[step % 2, piece], recv_sem=recv_sem.at[step % 2, piece],
            device_id={"py": to}, device_id_type=MESH,
        )

    def columns(count, sem):
        cells = speed.at[pl.ds(0, count // ni), :, inner(0)]
        return pltpu.make_async_copy(cells, cells, sem)

    def send_faces(step, piece, sides=SIDES):
        for side in sides:
            if side not in ends:
                face(step, piece, side).start()
                continue

            @pl.when(ends[side])
            def _():
                for part in (ROUND, BESIDE):
                    face(step, piece, side, part, passed=True).start()
                face(step, piece, side, STRAIGHT).start()

            @pl.when(jnp.logical_not(ends[side]))
            def _():
                face(step, piece, side).start()

    def as_relay(act):
        for (side, part), steps in away.items():
            at = (run - 1 if side == JUP else 0) + steps
            pl.when(place == at)(functools.partial(act, side, part))

    def relay(step, piece):
        def act(side, part):
            if step >= 2:
                pass_on(step - 2, piece, side, part).wait_send()
            face(step, piece, side, part, passed=True).wait_recv()
            pass_on(step, piece, side, part).start()

        as_relay(act)

    def k_face(step, high):
        return pltpu.make_async_remote_copy(
            src_ref=k_out.at[step % 2, high], dst_ref=k_in.at[step % 2, high],
            send_sem=k_send_sem.at[step % 2, high], recv_sem=k_recv_sem.at[step % 2, high],
            device_id={"pz": (up if high else down)["pz"]}, device_id_type=MESH,
        )

    def gather_k_face(step, high):
        slot = step % 2
        row = PAD + (nk - 1 if high else 0)

        def gather(j, _):
            for i in range(ni):
                k_out[slot, high, j, pl.ds(i, 1)] = field[slot, j + 1, i + 1, pl.ds(row, 1)]
            return 0

        lax.fori_loop(0, nj, gather, 0)

    def take_k_face(step, high):
        slot = step % 2
        row = PAD - 1 if high else PAD + nk
        k_face(step, high).wait_recv()

        def scatter(j, _):
            for i in range(ni):
                field[slot, j + 1, i + 1, pl.ds(row, 1)] = k_in[slot, high, j, pl.ds(i, 1)]
            return 0

        lax.fori_loop(0, nj, scatter, 0)

    def advance(step, piece):
        now, later = step % 2, (step + 1) % 2
        rows = padded(piece)
        lower, upper = padded(piece, -1), padded(piece, 1)

        def column(i, _):
            cells = [field[now, j, i + 1, rows] for j in range(nj + 2)]
            amount = None
            for j in range(1, nj + 1):
                middle = cells[j]
                spread = cells[j - 1] + cells[j + 1]
                spread = spread + (field[now, j, i, rows] + field[now, j, i + 2, rows])
                spread = spread + (field[now, j, i + 1, lower] + field[now, j, i + 1, upper])
                spread = spread - 6.0 * middle
                value = 2.0 * middle - field[later, j, i + 1, rows] + speed[j - 1, i, inner(piece)] * spread
                field[later, j, i + 1, rows] = value
                amount = value if amount is None else amount + value
            if step == STEPS - 1:
                total[i, inner(piece)] = amount
            return 0

        lax.fori_loop(0, ni, column, 0)

    def end_copy(piece):
        return pltpu.make_async_copy(
            field.at[STEPS % 2, pl.ds(1, nj), pl.ds(1, ni), padded(piece)], end_hbm.at[:, :, inner(piece)], out_sem.at[0]
        )

    def total_copy(piece, away):
        to = lax.rem(y + away, ny)
        return pltpu.make_async_remote_copy(
            src_ref=total.at[to, inner(piece)], dst_ref=gathered.at[piece, y],
            send_sem=t_send_sem, recv_sem=t_recv_sem.at[piece],
            device_id={"py": to}, device_id_type=MESH,
        )

    def prefix_copy(piece, away):
        to = lax.rem(y + away, ny)
        return pltpu.make_async_remote_copy(
            src_ref=prefix.at[piece, to], dst_ref=below_hbm.at[y, inner(piece)],
            send_sem=p_send_sem, recv_sem=p_recv_sem,
            device_id={"py": to}, device_id_type=MESH,
        )

    def own_prefix(piece):
        return pltpu.make_async_copy(prefix.at[piece, y], below_hbm.at[y, inner(piece)], out_sem.at[1])

    def others(sem):
        return pltpu.make_async_copy(gathered.at[0, pl.ds(0, ny - 1)], gathered.at[0, pl.ds(0, ny - 1)], sem)

    def to_all(copy, piece):
        def one(away, _):
            copy(piece, away).start()
            return 0

        lax.fori_loop(1, ny, one, 0)

    def send_totals(piece):
        to_all(total_copy, piece)

    def send_prefixes(piece):
        others(t_recv_sem.at[piece]).wait()
        gathered[piece, y] = total[y, inner(piece)]

        def add(n, so_far):
            prefix[piece, n] = so_far
            return so_far + gathered[piece, n]

        lax.fori_loop(0, ny, add, jnp.zeros(gathered.shape[2:], jnp.float32))
        to_all(prefix_copy, piece)
        own_prefix(piece).start()

    barrier = pltpu.get_barrier_semaphore()

    def greet(away, _):
        pl.semaphore_signal(barrier, inc=1, device_id={"py": lax.rem(y + away, ny)}, device_id_type=MESH)
        return 0

    for axis in ("px", "pz"):
        for near in (up, down):
            pl.semaphore_signal(barrier, inc=1, device_id={axis: near[axis]}, device_id_type=MESH)
    lax.fori_loop(1, ny, greet, 0)
    for which in range(3):
        for piece in ORDER:
            load(which, piece).start()
    loaded(0)
    for high in (0, 1):
        gather_k_face(0, high)
    pl.semaphore_wait(barrier, ny - 1 + 4)

    for high in (0, 1):
        k_face(0, high).start()
    for at, piece in enumerate(ORDER):
        if at >= 2:
            relay(0, ORDER[at - 2])
        send_faces(0, piece, SIDES if at < 2 else (JUP, JDOWN))

    for step in range(STEPS):
        for at, piece in enumerate(ORDER):
            if step == 0 and at == 0:
                loaded(1)
                loaded(2)
            if piece == 0:
                take_k_face(step, 1)
            if piece == CHUNKS - 1:
                take_k_face(step, 0)
            if step >= 1:
                relay(step, piece)
            elif at in (1, 2):
                relay(step, ORDER[at + 1])
            if step == STEPS - 1 and at == CHUNKS - 1:
                send_prefixes(ORDER[0])
            if step >= 1:
                columns(2 * (nj + ni), send_sem.at[(step - 1) % 2, piece]).wait()
            if step == 0 and at == 0:
                for n in (0, 1):
                    columns(2 * nj, i_recv_sem.at[0, ORDER[n]]).wait()
                    send_faces(0, ORDER[n + 2], (IUP, IDOWN))
            elif step >= 1 or at >= 2:
                columns(2 * nj, i_recv_sem.at[step % 2, piece]).wait()
            columns(2 * ni, recv_sem.at[step % 2, piece]).wait()
            advance(step, piece)
            if step < STEPS - 1:
                for high, owner in ((0, 0), (1, CHUNKS - 1)):
                    if piece == owner:
                        if step >= 1:
                            k_face(step - 1, high).wait_send()
                        gather_k_face(step + 1, high)
                        k_face(step + 1, high).start()
                send_faces(step + 1, piece)
            else:
                end_copy(piece).start()
                send_totals(piece)
    for piece in ORDER[1:]:
        send_prefixes(piece)
    for piece in ORDER:
        columns(2 * (nj + ni), send_sem.at[(STEPS - 1) % 2, piece]).wait()
    pltpu.make_async_copy(speed, end_hbm, out_sem.at[0]).wait()
    pltpu.make_async_copy(total.at[0], total.at[0], out_sem.at[1]).wait()
    for sem in (t_send_sem, p_send_sem, p_recv_sem):
        all_others = gathered.at[:, pl.ds(0, ny - 1)]
        pltpu.make_async_copy(all_others, all_others, sem).wait()
    for step in (STEPS - 2, STEPS - 1):
        for high in (0, 1):
            k_face(step, high).wait_send()

    def passed_on(side, part):
        for step in (STEPS - 2, STEPS - 1):
            for piece in ORDER:
                pass_on(step, piece, side, part).wait_send()

    as_relay(passed_on)


def sums_kernel(scale, field_ref, below_ref, sums_hbm, end_hbm, sums, sem):
    nj, ni = field_ref.shape[:2]
    ends = pltpu.make_async_copy(field_ref, end_hbm, sem.at[ni])
    ends.start()

    def put(i):
        return pltpu.make_async_copy(sums.at[:, i], sums_hbm.at[:, i], sem.at[i])

    def row(i, _):
        so_far = below_ref[i]
        for j in range(nj):
            so_far = so_far + field_ref[j, i]
            sums[j, i] = so_far * scale
        put(i).start()
        return 0

    lax.fori_loop(0, ni, row, 0)

    def written(i, _):
        put(i).wait()
        return 0

    lax.fori_loop(0, ni, written, 0)
    ends.wait()


def local(sizes, field_now, earlier, speed_square):
    nj, ni, nk, lanes = field_now.shape
    kc = nk // CHUNKS
    f32 = jnp.float32
    dma = pltpu.SemaphoreType.DMA
    end, below = pl.pallas_call(
        functools.partial(march_kernel, sizes),
        out_shape=(jax.ShapeDtypeStruct(field_now.shape, f32), jax.ShapeDtypeStruct((ni, nk, lanes), f32)),
        in_specs=[pl.BlockSpec(memory_space=pl.ANY)] * 3,
        out_specs=[pl.BlockSpec(memory_space=pl.ANY)] * 2,
        scratch_shapes=[
            pltpu.VMEM((2, nj + 2, ni + 2, nk + 2 * PAD, lanes), f32),
            pltpu.VMEM((nj, ni, nk, lanes), f32),
            pltpu.VMEM((2, 2, nj, ni, lanes), f32),
            pltpu.VMEM((2, 2, nj, ni, lanes), f32),
            pltpu.VMEM((ni, nk, lanes), f32),
            pltpu.VMEM((CHUNKS, ni, kc, lanes), f32),
            pltpu.VMEM((CHUNKS, ni, kc, lanes), f32),
            pltpu.VMEM((STEPS, CHUNKS, max(ROUND[1], BESIDE[1]), kc, lanes), f32),
            dma((3,)),
            dma((2, CHUNKS)),
            dma((2, CHUNKS)),
            dma((2, CHUNKS)),
            dma((2, 2)),
            dma((2, 2)),
            dma((2, CHUNKS)),
            dma((2, CHUNKS)),
            dma((2,)),
            dma,
            dma((CHUNKS,)),
            dma,
            dma,
        ],
        compiler_params=pltpu.CompilerParams(
            collective_id=0, has_side_effects=True, vmem_limit_bytes=48 * 1024 * 1024
        ),
        name="march",
    )(field_now, earlier, speed_square)
    sums, end = pl.pallas_call(
        functools.partial(sums_kernel, 1.0 / (nj * sizes[0])),
        out_shape=(jax.ShapeDtypeStruct(field_now.shape, f32),) * 2,
        in_specs=[pl.BlockSpec(memory_space=pltpu.VMEM)] * 2,
        out_specs=[pl.BlockSpec(memory_space=pl.ANY)] * 2,
        scratch_shapes=[pltpu.VMEM(field_now.shape, f32), dma((ni + 1,))],
        compiler_params=pltpu.CompilerParams(vmem_limit_bytes=16 * 1024 * 1024),
        name="sums",
    )(end, below)
    return sums, end


def solution(mesh):
    spec = P("py", "px", "pz", None)
    sizes = tuple(mesh.shape[axis] for axis in ("py", "px", "pz"))
    return jax.shard_map(
        functools.partial(local, sizes),
        mesh=mesh,
        in_specs=(spec, spec, spec),
        out_specs=(spec, spec),
        check_vma=False,
    )
```

```python
import functools

import jax
import jax.numpy as jnp
from jax import lax
from jax.experimental import pallas as pl
from jax.experimental.pallas import tpu as pltpu
from jax.sharding import PartitionSpec as P

STEPS = 4
MESH = pl.DeviceIdType.MESH
PAD = 8
CHUNKS = 4
ORDER = (1, 2, 0, 3)
JUP, JDOWN, IUP, IDOWN = SIDES = range(4)
STRAIGHT, ROUND, BESIDE = PARTS = ((0, 7), (7, 5), (12, 4))


def march_kernel(
    sizes, u_hbm, e_hbm, c_hbm, end_hbm, below_hbm,
    field, speed, k_out, k_in, total, gathered, prefix, passing,
    load_sem, send_sem, recv_sem, i_recv_sem, k_send_sem, k_recv_sem, pass_send_sem, pass_recv_sem,
    out_sem, t_send_sem, t_recv_sem, p_send_sem, p_recv_sem,
):
    ny, nx, nz = sizes
    nj, ni, nk, _ = u_hbm.shape
    kc = nk // CHUNKS
    y, x, z = lax.axis_index("py"), lax.axis_index("px"), lax.axis_index("pz")
    up = {"py": lax.rem(y + 1, ny), "px": lax.rem(x + 1, nx), "pz": lax.rem(z + 1, nz)}
    down = {"py": lax.rem(y + ny - 1, ny), "px": lax.rem(x + nx - 1, nx), "pz": lax.rem(z + nz - 1, nz)}

    def inner(piece):
        return pl.ds(piece * kc, kc)

    def padded(piece, shift=0):
        return pl.ds(PAD + piece * kc + shift, kc)

    def load(which, piece):
        block = (pl.ds(1, nj), pl.ds(1, ni), padded(piece))
        cells = (slice(None), slice(None), inner(piece))
        source = (u_hbm, e_hbm, c_hbm)[which].at[cells]
        target = speed.at[cells] if which == 2 else field.at[(which, *block)]
        return pltpu.make_async_copy(source, target, load_sem.at[which])

    run, half = ny // 2, ny // 4
    place = lax.rem(y, run)
    ends = {JUP: place == run - 1, JDOWN: place == 0}
    away = {(JUP, ROUND): 1 - half, (JUP, BESIDE): -half - 1, (JDOWN, ROUND): half - 1, (JDOWN, BESIDE): half + 1}

    def loaded(which):
        pltpu.make_async_copy(c_hbm, speed, load_sem.at[which]).wait()

    def face(step, piece, side, part=None, passed=False):
        slot = step % 2
        rows = padded(piece)
        first, count = part or (0, ni)
        i_all, j_all = pl.ds(1 + first, count), pl.ds(1, nj)
        along_j, high = side in (JUP, JDOWN), side in (JUP, IUP)
        if along_j:
            here = (slot, nj if high else 1, i_all, rows)
            there = (slot, 0 if high else nj + 1, i_all, rows)
        else:
            here = (slot, j_all, ni if high else 1, rows)
            there = (slot, j_all, 0 if high else ni + 1, rows)
        axis = "py" if along_j else "px"
        to = (up if high else down)[axis]
        source, target = field.at[here], field.at[there]
        arrived = (recv_sem if along_j else i_recv_sem).at[step % 2, piece]
        if passed:
            to = y + away[side, part]
            target, arrived = passing.at[step, piece, pl.ds(0, count)], pass_recv_sem.at[step % 2, piece]
        return pltpu.make_async_remote_copy(
            src_ref=source, dst_ref=target, send_sem=send_sem.at[step % 2, piece], recv_sem=arrived,
            device_id={axis: to}, device_id_type=MESH,
        )

    def pass_on(step, piece, side, part):
        first, count = part
        high = side == JUP
        to = lax.rem(y - away[side, part] + (1 if high else ny - 1), ny)
        there = (step % 2, 0 if high else nj + 1, pl.ds(1 + first, count), padded(piece))
        return pltpu.make_async_remote_copy(
            src_ref=passing.at[step, piece, pl.ds(0, count)], dst_ref=field.at[there],
            send_sem=pass_send_sem.at[step % 2, piece], recv_sem=recv_sem.at[step % 2, piece],
            device_id={"py": to}, device_id_type=MESH,
        )

    def columns(count, sem):
        cells = speed.at[pl.ds(0, count // ni), :, inner(0)]
        return pltpu.make_async_copy(cells, cells, sem)

    def send_parts(step, piece, side):
        for part in (ROUND, BESIDE):
            face(step, piece, side, part, passed=True).start()

    def send_faces(step, piece, sides=SIDES):
        for side in sides:
            if side not in ends:
                face(step, piece, side).start()
                continue

            @pl.when(ends[side])
            def _():
                if step >= 1:
                    send_parts(step, piece, side)
                face(step, piece, side, STRAIGHT).start()

            @pl.when(jnp.logical_not(ends[side]))
            def _():
                face(step, piece, side).start()

    def as_relay(act):
        for (side, part), steps in away.items():
            at = (run - 1 if side == JUP else 0) + steps
            pl.when(place == at)(functools.partial(act, side, part))

    def relay(step, piece):
        def act(side, part):
            if step >= 2:
                pass_on(step - 2, piece, side, part).wait_send()
            face(step, piece, side, part, passed=True).wait_recv()
            pass_on(step, piece, side, part).start()

        as_relay(act)

    def k_face(step, high):
        return pltpu.make_async_remote_copy(
            src_ref=k_out.at[step % 2, high], dst_ref=k_in.at[step % 2, high],
            send_sem=k_send_sem.at[step % 2, high], recv_sem=k_recv_sem.at[step % 2, high],
            device_id={"pz": (up if high else down)["pz"]}, device_id_type=MESH,
        )

    def gather_k_face(step, high):
        slot = step % 2
        row = PAD + (nk - 1 if high else 0)

        def gather(j, _):
            for i in range(ni):
                k_out[slot, high, j, pl.ds(i, 1)] = field[slot, j + 1, i + 1, pl.ds(row, 1)]
            return 0

        lax.fori_loop(0, nj, gather, 0)

    def take_k_face(step, high):
        slot = step % 2
        row = PAD - 1 if high else PAD + nk
        k_face(step, high).wait_recv()

        def scatter(j, _):
            for i in range(ni):
                field[slot, j + 1, i + 1, pl.ds(row, 1)] = k_in[slot, high, j, pl.ds(i, 1)]
            return 0

        lax.fori_loop(0, nj, scatter, 0)

    def advance(step, piece):
        now, later = step % 2, (step + 1) % 2
        rows = padded(piece)
        lower, upper = padded(piece, -1), padded(piece, 1)

        def column(i, _):
            cells = [field[now, j, i + 1, rows] for j in range(nj + 2)]
            amount = None
            for j in range(1, nj + 1):
                middle = cells[j]
                spread = cells[j - 1] + cells[j + 1]
                spread = spread + (field[now, j, i, rows] + field[now, j, i + 2, rows])
                spread = spread + (field[now, j, i + 1, lower] + field[now, j, i + 1, upper])
                spread = spread - 6.0 * middle
                value = 2.0 * middle - field[later, j, i + 1, rows] + speed[j - 1, i, inner(piece)] * spread
                field[later, j, i + 1, rows] = value
                amount = value if amount is None else amount + value
            if step == STEPS - 1:
                total[i, inner(piece)] = amount
            return 0

        lax.fori_loop(0, ni, column, 0)

    def end_copy(piece):
        return pltpu.make_async_copy(
            field.at[STEPS % 2, pl.ds(1, nj), pl.ds(1, ni), padded(piece)], end_hbm.at[:, :, inner(piece)], out_sem.at[0]
        )

    def total_copy(piece, away):
        to = lax.rem(y + away, ny)
        return pltpu.make_async_remote_copy(
            src_ref=total.at[to, inner(piece)], dst_ref=gathered.at[piece, y],
            send_sem=t_send_sem, recv_sem=t_recv_sem.at[piece],
            device_id={"py": to}, device_id_type=MESH,
        )

    def prefix_copy(piece, away):
        to = lax.rem(y + away, ny)
        return pltpu.make_async_remote_copy(
            src_ref=prefix.at[piece, to], dst_ref=below_hbm.at[y, inner(piece)],
            send_sem=p_send_sem, recv_sem=p_recv_sem,
            device_id={"py": to}, device_id_type=MESH,
        )

    def own_prefix(piece):
        return pltpu.make_async_copy(prefix.at[piece, y], below_hbm.at[y, inner(piece)], out_sem.at[1])

    def others(sem):
        return pltpu.make_async_copy(gathered.at[0, pl.ds(0, ny - 1)], gathered.at[0, pl.ds(0, ny - 1)], sem)

    def to_all(copy, piece):
        def one(away, _):
            copy(piece, away).start()
            return 0

        lax.fori_loop(1, ny, one, 0)

    def send_totals(piece):
        to_all(total_copy, piece)

    def send_prefixes(piece):
        others(t_recv_sem.at[piece]).wait()
        gathered[piece, y] = total[y, inner(piece)]

        def add(n, so_far):
            prefix[piece, n] = so_far
            return so_far + gathered[piece, n]

        lax.fori_loop(0, ny, add, jnp.zeros(gathered.shape[2:], jnp.float32))
        to_all(prefix_copy, piece)
        own_prefix(piece).start()

    barrier = pltpu.get_barrier_semaphore()

    def greet(away, _):
        pl.semaphore_signal(barrier, inc=1, device_id={"py": lax.rem(y + away, ny)}, device_id_type=MESH)
        return 0

    for axis in ("px", "pz"):
        for near in (up, down):
            pl.semaphore_signal(barrier, inc=1, device_id={axis: near[axis]}, device_id_type=MESH)
    lax.fori_loop(1, ny, greet, 0)
    for which in range(3):
        for piece in ORDER:
            load(which, piece).start()
    loaded(0)
    for high in (0, 1):
        gather_k_face(0, high)
    pl.semaphore_wait(barrier, ny - 1 + 4)

    for high in (0, 1):
        k_face(0, high).start()
    for side, here in ends.items():

        @pl.when(here)
        def _():
            for piece in ORDER:
                send_parts(0, piece, side)

    for at, piece in enumerate(ORDER):
        if at >= 2:
            relay(0, ORDER[at - 2])
        send_faces(0, piece, SIDES if at < 2 else (JUP, JDOWN))

    for step in range(STEPS):
        for at, piece in enumerate(ORDER):
            if step == 0 and at == 0:
                loaded(1)
                loaded(2)
            if piece == 0:
                take_k_face(step, 1)
            if piece == CHUNKS - 1:
                take_k_face(step, 0)
            if step >= 1:
                relay(step, piece)
            elif at in (1, 2):
                relay(step, ORDER[at + 1])
            if step == STEPS - 1 and at == CHUNKS - 1:
                send_prefixes(ORDER[0])
            if step >= 1:
                columns(2 * (nj + ni), send_sem.at[(step - 1) % 2, piece]).wait()
            if step == 0 and at == 0:
                for n in (0, 1):
                    columns(2 * nj, i_recv_sem.at[0, ORDER[n]]).wait()
                    send_faces(0, ORDER[n + 2], (IUP, IDOWN))
            elif step >= 1 or at >= 2:
                columns(2 * nj, i_recv_sem.at[step % 2, piece]).wait()
            columns(2 * ni, recv_sem.at[step % 2, piece]).wait()
            advance(step, piece)
            if step < STEPS - 1:
                for high, owner in ((0, 0), (1, CHUNKS - 1)):
                    if piece == owner:
                        if step >= 1:
                            k_face(step - 1, high).wait_send()
                        gather_k_face(step + 1, high)
                        k_face(step + 1, high).start()
                send_faces(step + 1, piece)
            else:
                end_copy(piece).start()
                send_totals(piece)
    for piece in ORDER[1:]:
        send_prefixes(piece)
    for piece in ORDER:
        columns(2 * (nj + ni), send_sem.at[(STEPS - 1) % 2, piece]).wait()
    pltpu.make_async_copy(speed, end_hbm, out_sem.at[0]).wait()
    pltpu.make_async_copy(total.at[0], total.at[0], out_sem.at[1]).wait()
    for sem in (t_send_sem, p_send_sem, p_recv_sem):
        all_others = gathered.at[:, pl.ds(0, ny - 1)]
        pltpu.make_async_copy(all_others, all_others, sem).wait()
    for step in (STEPS - 2, STEPS - 1):
        for high in (0, 1):
            k_face(step, high).wait_send()

    def passed_on(side, part):
        for step in (STEPS - 2, STEPS - 1):
            for piece in ORDER:
                pass_on(step, piece, side, part).wait_send()

    as_relay(passed_on)


def sums_kernel(scale, field_ref, below_ref, sums_hbm, end_hbm, sums, sem):
    nj, ni = field_ref.shape[:2]
    ends = pltpu.make_async_copy(field_ref, end_hbm, sem.at[ni])
    ends.start()

    def put(i):
        return pltpu.make_async_copy(sums.at[:, i], sums_hbm.at[:, i], sem.at[i])

    def row(i, _):
        so_far = below_ref[i]
        for j in range(nj):
            so_far = so_far + field_ref[j, i]
            sums[j, i] = so_far * scale
        put(i).start()
        return 0

    lax.fori_loop(0, ni, row, 0)

    def written(i, _):
        put(i).wait()
        return 0

    lax.fori_loop(0, ni, written, 0)
    ends.wait()


def local(sizes, field_now, earlier, speed_square):
    nj, ni, nk, lanes = field_now.shape
    kc = nk // CHUNKS
    f32 = jnp.float32
    dma = pltpu.SemaphoreType.DMA
    end, below = pl.pallas_call(
        functools.partial(march_kernel, sizes),
        out_shape=(jax.ShapeDtypeStruct(field_now.shape, f32), jax.ShapeDtypeStruct((ni, nk, lanes), f32)),
        in_specs=[pl.BlockSpec(memory_space=pl.ANY)] * 3,
        out_specs=[pl.BlockSpec(memory_space=pl.ANY)] * 2,
        scratch_shapes=[
            pltpu.VMEM((2, nj + 2, ni + 2, nk + 2 * PAD, lanes), f32),
            pltpu.VMEM((nj, ni, nk, lanes), f32),
            pltpu.VMEM((2, 2, nj, ni, lanes), f32),
            pltpu.VMEM((2, 2, nj, ni, lanes), f32),
            pltpu.VMEM((ni, nk, lanes), f32),
            pltpu.VMEM((CHUNKS, ni, kc, lanes), f32),
            pltpu.VMEM((CHUNKS, ni, kc, lanes), f32),
            pltpu.VMEM((STEPS, CHUNKS, max(ROUND[1], BESIDE[1]), kc, lanes), f32),
            dma((3,)),
            dma((2, CHUNKS)),
            dma((2, CHUNKS)),
            dma((2, CHUNKS)),
            dma((2, 2)),
            dma((2, 2)),
            dma((2, CHUNKS)),
            dma((2, CHUNKS)),
            dma((2,)),
            dma,
            dma((CHUNKS,)),
            dma,
            dma,
        ],
        compiler_params=pltpu.CompilerParams(
            collective_id=0, has_side_effects=True, vmem_limit_bytes=48 * 1024 * 1024
        ),
        name="march",
    )(field_now, earlier, speed_square)
    sums, end = pl.pallas_call(
        functools.partial(sums_kernel, 1.0 / (nj * sizes[0])),
        out_shape=(jax.ShapeDtypeStruct(field_now.shape, f32),) * 2,
        in_specs=[pl.BlockSpec(memory_space=pltpu.VMEM)] * 2,
        out_specs=[pl.BlockSpec(memory_space=pl.ANY)] * 2,
        scratch_shapes=[pltpu.VMEM(field_now.shape, f32), dma((ni + 1,))],
        compiler_params=pltpu.CompilerParams(vmem_limit_bytes=16 * 1024 * 1024),
        name="sums",
    )(end, below)
    return sums, end


def solution(mesh):
    spec = P("py", "px", "pz", None)
    sizes = tuple(mesh.shape[axis] for axis in ("py", "px", "pz"))
    return jax.shard_map(
        functools.partial(local, sizes),
        mesh=mesh,
        in_specs=(spec, spec, spec),
        out_specs=(spec, spec),
        check_vma=False,
    )
```
